32 devices in a mesh: grp: 2 (over y), smp: 4 (over z), trm: 2 (over x), sub: 2 (over core).
Axes of the slice: x: 2, y: 2, z: 4, core: 2. Of those that a mesh axis runs over, the one named last changes fastest.
Arguments:
- inputs: float32 [20, 8192], P(None, ('grp', 'smp', 'sub')), parts along dimension 1, may hold values from -1 to 1
- weights: float32 [8192], P(('grp', 'smp', 'sub')), parts along dimension 0, may hold values from 0.25 to 4
- response: float32 [8192], P(('grp', 'smp', 'sub')), parts along dimension 0, may hold values from 0.5 to 3
- index_table: int32 [20, 1792], P(None, 'trm'), may hold values from 0 to 3, as said below
Outputs:
- gram: float32 [3584, 1792], P(('grp', 'trm'), ('smp', 'sub')), parts along dimension 0
- rhs: float32 [3584], P(('grp', 'trm')), parts along dimension 0
The draws below stay inside these ranges and needn't reach their ends.
There are 2 independent parts, one for each index of `grp`. The reference program is written for one: setup_inputs(seed, part) draws one part's arguments, and reference() takes and returns one part's arrays. A program takes and returns all parts, laid end to end along the dimension named above; an argument that names none is the same for every part. Nothing has to cross between parts.
Inputs may be any that keep to these rules, and one draw needn't show every extreme that they name: `index_table`: each column holds the degrees of a multi-index of total degree at most 3. No multi-index other than the all-zero one stands in two columns; when 1792 is 1771 or more, every multi-index of total degree at most 3 over 20 inputs stands in some column.
All inputs are finite; a program needn't handle non-finite values.
Results may differ from the reference program's by a relative error of at most 0.00043.
Values may be sent and summed in bfloat16 or wider, within the bound.
A program may use at most 64 MiB of HBM per device.

```python
import math
import jax
import jax.numpy as jnp
import numpy as np
from jax import lax

NIN = 20
TERMS = 1792
S_DEV = 512
SAMPLES = 4096


def draw_inputs(key, part):
    uniform = jax.random.uniform(jax.random.fold_in(key, 11), (NIN, SAMPLES), jnp.float32)
    values = -1.0 + 2.0 * uniform * uniform
    return jnp.clip(values, -1.0, 1.0).astype(jnp.float32)


def index_enumeration():
    columns = []
    cube_list = []
    for first_pick in range(NIN + 1):
        for second_pick in range(first_pick, NIN + 1):
            for third_pick in range(second_pick, NIN + 1):
                counts = np.zeros(NIN, np.int32)
                for picked in (first_pick, second_pick, third_pick):
                    if picked < NIN:
                        counts[picked] += 1
                if first_pick == third_pick and first_pick < NIN:
                    cube_list.append(len(columns))
                columns.append(counts)
    return (np.stack(columns, axis=1), np.array(cube_list, np.int32))


def draw_index_table(key, part):
    table, cube_list = index_enumeration()
    distinct = table.shape[1]
    total = max(TERMS, distinct)
    padded = np.concatenate([table, np.zeros((NIN, total - distinct), np.int32)], axis=1)
    order = jax.random.permutation(jax.random.fold_in(key, 23), total).astype(jnp.int32)
    chosen_cube = jnp.asarray(cube_list)[jax.random.randint(jax.random.fold_in(key, 29), (), 0, NIN)]
    target = jax.random.randint(jax.random.fold_in(key, 31), (), 0, TERMS).astype(jnp.int32)
    where_cube = jnp.argmax(order == chosen_cube).astype(jnp.int32)
    displaced = order[target]
    order = order.at[where_cube].set(displaced).at[target].set(chosen_cube)
    return jnp.asarray(padded)[:, order[:TERMS]].astype(jnp.int32)


def level_of(own_key, shape, split, low, top_value):
    loudness, own = 1.0, jax.random.fold_in(own_key, 6)
    for dim, shards_of in split:
        draws = jnp.exp(jax.random.uniform(jax.random.fold_in(own, dim), (shards_of,), jnp.float32, low / len(split), top_value / len(split)))
        loudness = loudness * jnp.repeat(draws, shape[dim] // shards_of).reshape([-1 if axis == dim else 1 for axis in range(len(shape))])
    return loudness


def setup_inputs(seed: int = 0, part: int = 0) -> dict:
    seeds = jax.random.split(jax.random.key(seed), 5)
    part_splits = jax.random.split(jax.random.fold_in(seeds[4], part), 5)
    return {
        "inputs": draw_inputs(jax.random.fold_in(jax.random.fold_in(seeds[4], part), 71), part),
        "weights": jnp.clip(jnp.exp(math.log(4.0) - 2.7725887 * jax.random.uniform(part_splits[1], (SAMPLES,), jnp.float32) ** level_of(part_splits[1], (SAMPLES,), ((0, 8),), -0.2, 0.2)), 0.25, 4.0),
        "response": jnp.clip(0.5 + 2.5 * jax.random.uniform(part_splits[2], (SAMPLES,), jnp.float32) ** level_of(part_splits[2], (SAMPLES,), ((0, 8),), -0.2, 0.2), 0.5, 3.0),
        "index_table": draw_index_table(jax.random.fold_in(seeds[4], 71), part),
    }


def legendre_values(values):
    first = jnp.sqrt(jnp.float32(3.0)) * values
    second = jnp.sqrt(jnp.float32(5.0)) * (1.5 * values * values - 0.5)
    third = jnp.sqrt(jnp.float32(7.0)) * (2.5 * values * values * values - 1.5 * values)
    return jnp.stack([jnp.ones_like(values), first, second, third], axis=0)

def design_block(block_inputs, index_table):
    levels = legendre_values(block_inputs)
    degrees = jnp.arange(4, dtype=jnp.int32)

    def one_input(j, product):
        values = lax.dynamic_index_in_dim(levels, j, 1, keepdims=False)
        column = lax.dynamic_index_in_dim(index_table, j, 0, keepdims=False)
        onehot = (column[None, :] == degrees[:, None]).astype(jnp.float32)
        picked = lax.optimization_barrier(jnp.sum(values[:, None, :] * onehot[:, :, None], axis=0))
        return product * picked
    start = jnp.ones((index_table.shape[1], block_inputs.shape[1]), jnp.float32)
    return lax.fori_loop(0, NIN, one_input, start)

def reference(inputs, weights, response, index_table):
    blocks = SAMPLES // S_DEV

    def one_block(b, carry):
        gram_acc, rhs_acc = carry
        begin = (b * S_DEV).astype(jnp.int32)
        block_inputs = lax.dynamic_slice_in_dim(inputs, begin, S_DEV, 1)
        block_weights = lax.dynamic_slice_in_dim(weights, begin, S_DEV, 0)
        block_response = lax.dynamic_slice_in_dim(response, begin, S_DEV, 0)
        design = design_block(block_inputs, index_table)
        design_b = design.astype(jnp.bfloat16)
        rooted = (design * jnp.sqrt(block_weights / SAMPLES)[None, :]).astype(jnp.bfloat16)
        scaled = (block_weights * block_response / SAMPLES).astype(jnp.bfloat16)
        gram_part = lax.dot_general(rooted, rooted, (((1,), (1,)), ((), ())), preferred_element_type=jnp.float32)
        rhs_part = jnp.dot(design_b, scaled, preferred_element_type=jnp.float32)
        return (gram_acc + gram_part, rhs_acc + rhs_part)
    start = (jnp.zeros((TERMS, TERMS), jnp.float32), jnp.zeros((TERMS,), jnp.float32))
    gram, rhs = lax.fori_loop(0, blocks, one_block, start)
    return (gram, rhs)
```

```python
import functools

import jax
import jax.numpy as jnp
from jax import lax
from jax.experimental import pallas as pl
from jax.experimental.pallas import tpu as pltpu
from jax.sharding import PartitionSpec as P

MESH = pl.DeviceIdType.MESH


def up8(n):
    return -(-n // 8) * 8


class Plan:
    def __init__(self, nin):
        self.nin = nin
        self.single = up8(nin + 1)
        self.slab = up8(nin + 2)
        self.pairs = up8(nin * (nin - 1) // 2)
        self.triple = {}
        row = 0
        for c in range(2, nin + 1):
            self.triple[c] = row
            row += up8(c * (c - 1) // 2)
        self.square = row
        row += nin * self.single
        self.linear = row
        row += self.single
        self.cube = row
        row += self.single
        self.rows = -(-row // 16) * 16


def positions(plan, degrees):
    total = jnp.zeros_like(degrees[0:1, :])
    first, second, third = total, total, total
    for j in range(plan.nin):
        total = total + degrees[j : j + 1, :]
        first = first + (total < 1).astype(jnp.int32)
        second = second + (total < 2).astype(jnp.int32)
        third = third + (total < 3).astype(jnp.int32)
    nin, single = plan.nin, plan.single
    offset = jnp.zeros_like(total)
    for c, start in plan.triple.items():
        offset = jnp.where(third == c, start, offset)
    code = offset + (second * (second - 1)) // 2 + first
    code = jnp.where(
        (first == second) & (second < third), plan.square + first * single + third, code
    )
    code = jnp.where(
        (first < second) & (second == third), plan.square + second * single + first, code
    )
    code = jnp.where((first == second) & (second == third), plan.cube + first, code)
    return jnp.where((second == nin) & (third == nin), plan.linear + first, code)


def build_left(plan, slab, q_ref, pair_ref, left_ref):
    nin, single = plan.nin, plan.single
    x = slab[0:single, :]
    root = slab[nin : nin + 1, :]
    rows = lax.broadcasted_iota(jnp.int32, x.shape, 0)
    q1 = jnp.where(rows < nin, jnp.sqrt(jnp.float32(3.0)) * x, (rows == nin).astype(jnp.float32))
    q2 = jnp.sqrt(jnp.float32(5.0)) * (1.5 * x * x - 0.5) * root
    q3 = jnp.sqrt(jnp.float32(7.0)) * (2.5 * x * x * x - 1.5 * x) * root
    q1_root = q1 * root
    q_ref[0:single, :] = q1
    q_ref[single : 2 * single, :] = q2
    for b in range(1, nin):
        at = b * (b - 1) // 2
        pair_ref[at : at + b, :] = q1_root[0:b, :] * q1[b : b + 1, :]
    blocks = []
    for c in range(2, nin + 1):
        for r in range(0, up8(c * (c - 1) // 2), 8):
            blocks.append(("pair", r, c))
    for c in range(nin):
        for r in range(0, single, 8):
            blocks.append(("one", r, c))
    for r in range(0, single, 8):
        blocks.append(("lin", r, 0))
    for r in range(0, single, 8):
        blocks.append(("cube", r, 0))

    def value(kind, r, c):
        if kind == "pair":
            v = pair_ref[r : r + 8, :]
            return v if c == nin else v * q_ref[c : c + 1, :]
        if kind == "one":
            return q_ref[r : r + 8, :] * q_ref[single + c : single + c + 1, :]
        return (q1_root if kind == "lin" else q3)[r : r + 8, :]

    for g in range(0, len(blocks), 2):
        low = value(*blocks[g])
        high = value(*blocks[g + 1]) if g + 1 < len(blocks) else jnp.zeros_like(low)
        left_ref[8 * g : 8 * g + 16, :] = jnp.concatenate([low, high], axis=0).astype(jnp.bfloat16)


def xor_index(a, b, n):
    if n & (n - 1):
        return lax.rem(a + b, n)
    out, bit = 0, 1
    while bit < n:
        out = out + bit * (((a // bit) % 2 + (b // bit) % 2) % 2)
        bit *= 2
    return out


def kernel(
    plan, sizes, columns, samples_total,
    x_ref, w_ref, y_ref, deg_ref, gram_ref, rhs_ref,
    slabs, code_ref, codes_in, code_smem, sel_ref, left_a, left_b, q_ref, pair_ref, acc, picked,
    ici_send, sub_send, recv, code_send, code_recv, smem_sem,
):
    nsmp, nsub, ntrm = sizes
    smp, sub, trm = lax.axis_index("smp"), lax.axis_index("sub"), lax.axis_index("trm")
    me = smp * nsub + sub
    single = plan.single
    terms = deg_ref.shape[1]
    width = acc.shape[1]

    barrier = pltpu.get_barrier_semaphore()
    for d in range(1, nsmp):
        pl.semaphore_signal(barrier, inc=1, device_id={"smp": xor_index(smp, d, nsmp)}, device_id_type=MESH)
    for d in range(1, nsub):
        pl.semaphore_signal(barrier, inc=1, device_id={"sub": lax.rem(sub + d, nsub)}, device_id_type=MESH)
    for d in range(1, ntrm):
        pl.semaphore_signal(barrier, inc=1, device_id={"trm": lax.rem(trm + d, ntrm)}, device_id_type=MESH)

    weights = w_ref[...]
    root = jnp.sqrt(weights / samples_total)
    scaled = (weights * y_ref[...] / samples_total).astype(jnp.bfloat16).astype(jnp.float32)
    mine = slabs.at[me]
    spare = plan.slab - plan.nin - 2
    mine[...] = jnp.concatenate(
        [x_ref[...], root, scaled / root, jnp.zeros((spare, x_ref.shape[1]), jnp.float32)], axis=0
    )
    code = positions(plan, deg_ref[...])
    code_ref[...] = code
    per_trm = terms // columns
    for k in range(per_trm):
        @pl.when(lax.rem(me, per_trm) == k)
        def _():
            part = code[:, k * columns : (k + 1) * columns].astype(jnp.float32)
            pad = jnp.full((1, width - columns), -1.0, jnp.float32)
            codes_in[trm] = jnp.broadcast_to(jnp.concatenate([part, pad], axis=1), (8, width))
    to_smem = pltpu.make_async_copy(code_ref, code_smem, smem_sem)
    to_smem.start()
    pair_ref[...] = jnp.zeros_like(pair_ref)
    acc[...] = jnp.zeros_like(acc)

    pl.semaphore_wait(barrier, (nsmp - 1) + (nsub - 1) + (ntrm - 1))

    def sub_copy(chunk, p, d):
        return pltpu.make_async_remote_copy(
            src_ref=slabs.at[chunk], dst_ref=slabs.at[chunk],
            send_sem=sub_send.at[p, d - 1], recv_sem=recv.at[chunk],
            device_id={"sub": lax.rem(sub + d, nsub)}, device_id_type=MESH,
        )

    def ici_copy(d):
        return pltpu.make_async_remote_copy(
            src_ref=slabs.at[me], dst_ref=slabs.at[me],
            send_sem=ici_send.at[d - 1], recv_sem=recv.at[me],
            device_id={"smp": xor_index(smp, d, nsmp)}, device_id_type=MESH,
        )

    def code_copy(d):
        return pltpu.make_async_remote_copy(
            src_ref=codes_in.at[trm], dst_ref=codes_in.at[trm],
            send_sem=code_send.at[d - 1], recv_sem=code_recv.at[trm],
            device_id={"trm": lax.rem(trm + d, ntrm)}, device_id_type=MESH,
        )

    def wait_slab(chunk):
        pltpu.make_async_remote_copy(
            src_ref=slabs.at[chunk], dst_ref=slabs.at[chunk],
            send_sem=ici_send.at[0], recv_sem=recv.at[chunk],
            device_id={"sub": lax.rem(sub + 1, nsub)}, device_id_type=MESH,
        ).wait_recv()

    for d in range(1, ntrm):
        code_copy(d).start()
    for d in range(1, nsub):
        sub_copy(me, 0, d).start()
    for d in range(1, nsmp):
        ici_copy(d).start()

    build_left(plan, slabs[me], q_ref, pair_ref, left_a)

    for d in range(1, ntrm):
        other = lax.rem(trm + d, ntrm)
        pltpu.make_async_remote_copy(
            src_ref=codes_in.at[other], dst_ref=codes_in.at[other],
            send_sem=code_send.at[d - 1], recv_sem=code_recv.at[other],
            device_id={"trm": other}, device_id_type=MESH,
        ).wait_recv()
    owner = me // per_trm
    wanted = codes_in[owner]
    for i in range(0, width, 128):
        column = jnp.broadcast_to(wanted[0:1, i : i + 128], (128, 128)).T.astype(jnp.int32)
        for j in range(0, sel_ref.shape[1], 128):
            cols = min(128, sel_ref.shape[1] - j)
            lane = lax.broadcasted_iota(jnp.int32, (128, cols), 1) + j
            sel_ref[i : i + 128, j : j + cols] = (column[:, :cols] == lane).astype(jnp.bfloat16)

    def chunk_of(p, s):
        return xor_index(smp, p, nsmp) * nsub + lax.rem(sub + s, nsub)

    def compute(chunk, left_ref):
        left = left_ref[...]
        right = lax.dot_general(
            sel_ref[...], left, (((1,), (0,)), ((), ())), preferred_element_type=jnp.float32
        )
        z = slabs[chunk][plan.nin + 1 : plan.nin + 2, :]
        high = z.astype(jnp.bfloat16).astype(jnp.float32)
        low = z - high
        rows = lax.broadcasted_iota(jnp.int32, right.shape, 0)
        right = jnp.where(rows == columns, high, jnp.where(rows == columns + 1, low, right))
        acc[...] += lax.dot_general(
            left, right.astype(jnp.bfloat16), (((1,), (1,)), ((), ())),
            preferred_element_type=jnp.float32,
        )

    def body(p, carry):
        second = chunk_of(p, 1)
        wait_slab(second)
        compute(chunk_of(p, 0), left_a)
        build_left(plan, slabs[second], q_ref, pair_ref, left_b)
        following = chunk_of(lax.rem(p + 1, nsmp), 0)

        @pl.when(p + 1 < nsmp)
        def _():
            wait_slab(following)
            for d in range(1, nsub):
                sub_copy(following, p + 1, d).start()

        compute(second, left_b)
        build_left(plan, slabs[following], q_ref, pair_ref, left_a)
        return carry

    lax.fori_loop(0, nsmp, body, 0)

    to_smem.wait()

    for base in range(0, terms, 128):
        count = min(128, terms - base)
        for r in range(base, base + count):
            picked[r : r + 1, :] = acc[pl.ds(code_smem[0, r], 1), :]
        turned = picked[base : base + count, :].T
        gram_ref[:, base : base + count] = turned[0:columns, :]
        rhs_ref[base // 128 : base // 128 + 1, 0:count] = (
            turned[columns : columns + 1, :] + turned[columns + 1 : columns + 2, :]
        )

    for d in range(1, ntrm):
        code_copy(d).wait_send()
    for d in range(1, nsmp):
        ici_copy(d).wait_send()
    for p in range(nsmp):
        for d in range(1, nsub):
            sub_copy(chunk_of(p, 0), p, d).wait_send()


def write_out(gram_ref, rhs_ref, gram_out, rhs_out, flat, sem):
    copy = pltpu.make_async_copy(gram_ref, gram_out, sem.at[0])
    copy.start()
    flat[...] = rhs_ref[...].reshape(flat.shape)
    line = pltpu.make_async_copy(flat.at[pl.ds(0, rhs_out.shape[0])], rhs_out, sem.at[1])
    line.start()
    line.wait()
    copy.wait()


def solution(mesh):
    nsmp, nsub, ntrm = mesh.shape["smp"], mesh.shape["sub"], mesh.shape["trm"]

    def local(inputs, weights, response, index_table):
        nin, samples = inputs.shape
        terms = index_table.shape[1]
        columns = terms * ntrm // (nsmp * nsub)
        plan = Plan(nin)
        width = -(-(columns + 2) // 128) * 128
        chunks = nsmp * nsub
        gram, rhs = pl.pallas_call(
            functools.partial(kernel, plan, (nsmp, nsub, ntrm), columns, samples * chunks),
            out_shape=(
                pltpu.VMEM((columns, terms), jnp.float32),
                pltpu.VMEM((up8(-(-terms // 128)), 128), jnp.float32),
            ),
            in_specs=[pl.BlockSpec(memory_space=pltpu.VMEM)] * 4,
            out_specs=(pl.BlockSpec(memory_space=pltpu.VMEM),) * 2,
            scratch_shapes=[
                pltpu.VMEM((chunks, plan.slab, samples), jnp.float32),
                pltpu.VMEM((1, terms), jnp.int32),
                pltpu.VMEM((ntrm, 8, width), jnp.float32),
                pltpu.SMEM((1, terms), jnp.int32),
                pltpu.VMEM((width, plan.rows), jnp.bfloat16),
                pltpu.VMEM((plan.rows, samples), jnp.bfloat16),
                pltpu.VMEM((plan.rows, samples), jnp.bfloat16),
                pltpu.VMEM((2 * plan.single, samples), jnp.float32),
                pltpu.VMEM((plan.pairs, samples), jnp.float32),
                pltpu.VMEM((plan.rows, width), jnp.float32),
                pltpu.VMEM((terms, width), jnp.float32),
                pltpu.SemaphoreType.DMA((max(nsmp - 1, 1),)),
                pltpu.SemaphoreType.DMA((nsmp, max(nsub - 1, 1))),
                pltpu.SemaphoreType.DMA((chunks,)),
                pltpu.SemaphoreType.DMA((max(ntrm - 1, 1),)),
                pltpu.SemaphoreType.DMA((ntrm,)),
                pltpu.SemaphoreType.DMA,
            ],
            compiler_params=pltpu.CompilerParams(
                collective_id=0, has_side_effects=True, vmem_limit_bytes=56 * 1024 * 1024
            ),
        )(inputs, weights.reshape(1, samples), response.reshape(1, samples), index_table)
        gram, rhs = pl.pallas_call(
            write_out,
            out_shape=(
                jax.ShapeDtypeStruct((columns, terms), jnp.float32),
                jax.ShapeDtypeStruct((rhs.size if terms % 128 else terms,), jnp.float32),
            ),
            in_specs=[pl.BlockSpec(memory_space=pltpu.VMEM)] * 2,
            out_specs=(pl.BlockSpec(memory_space=pl.ANY),) * 2,
            scratch_shapes=[
                pltpu.VMEM((rhs.size,), jnp.float32),
                pltpu.SemaphoreType.DMA((2,)),
            ],
        )(
            pltpu.with_memory_space_constraint(gram, pltpu.VMEM),
            pltpu.with_memory_space_constraint(rhs, pltpu.VMEM),
        )
        return gram.T, rhs[0:terms]

    return jax.shard_map(
        local,
        mesh=mesh,
        in_specs=(
            P(None, ("grp", "smp", "sub")),
            P(("grp", "smp", "sub")),
            P(("grp", "smp", "sub")),
            P(None, "trm"),
        ),
        out_specs=(P(("grp", "trm"), ("smp", "sub")), P(("grp", "trm"))),
        check_vma=False,
    )
```

```python
import functools
import math

import jax
import jax.numpy as jnp
from jax import lax
from jax.experimental import pallas as pl
from jax.experimental.pallas import tpu as pltpu
from jax.sharding import PartitionSpec as P

MESH = pl.DeviceIdType.MESH
BASE = 256


def up(n, m):
    return -(-n // m) * m


class Plan:
    def __init__(self, nin):
        self.nin = nin
        self.half = nin // 2
        self.single = up(nin + 1, 8)
        self.slab = up(nin + 2, 8)
        self.q2 = self.single
        self.q3 = self.single + nin
        self.rows_a = max(up(self.single + 2 * nin, 16), 64)
        self.low = self.single
        self.high = self.low + self.half * (self.half - 1) // 2
        rest = nin - self.half
        self.rows_b = max(up(self.high + rest * (rest - 1) // 2, 16), 128)


def positions(plan, degrees):
    total = jnp.zeros_like(degrees[0:1, :])
    first, second, third = total, total, total
    for j in range(plan.nin):
        total = total + degrees[j : j + 1, :]
        first = first + (total < 1).astype(jnp.int32)
        second = second + (total < 2).astype(jnp.int32)
        third = third + (total < 3).astype(jnp.int32)
    nin, half = plan.nin, plan.half
    low = second < half
    big = jnp.where(low, second, third - half)
    small = jnp.where(low, first, second - half)
    pair = jnp.where(low, plan.low, plan.high) + (big * (big - 1)) // 2 + small
    a = jnp.where(low, third, first)
    b = pair
    twin = (first == second) | (second == third)
    a = jnp.where(twin, plan.q2 + second, a)
    b = jnp.where(twin, jnp.where(first == second, third, first), b)
    triple = (first == second) & (second == third)
    a = jnp.where(triple, plan.q3 + first, a)
    b = jnp.where(triple, nin, b)
    a = jnp.where((third == nin) & (first != second), first, a)
    b = jnp.where((third == nin) & (first != second), second, b)
    a = jnp.where(first == nin, nin, a)
    b = jnp.where(first == nin, nin, b)
    return a * BASE + b


def split(v):
    high = v.astype(jnp.bfloat16)
    return high, (v - high.astype(jnp.float32)).astype(jnp.bfloat16)


def build_tables(plan, samples_total, slab, work, ta, tb, z_ref):
    nin, single = plan.nin, plan.single
    x = slab[0:single, :]
    weights = slab[nin : nin + 1, :]
    root = jnp.sqrt(weights / samples_total)
    scaled = weights * slab[nin + 1 : nin + 2, :] / samples_total
    z_high, z_low = split(scaled.astype(jnp.bfloat16).astype(jnp.float32) / root)
    z_ref[...] = jnp.concatenate(
        [z_high.astype(jnp.float32), z_low.astype(jnp.float32), jnp.zeros((14, x.shape[1]), jnp.float32)], axis=0
    ).astype(jnp.bfloat16)
    rows = lax.broadcasted_iota(jnp.int32, x.shape, 0)
    q1 = jnp.where(rows < nin, math.sqrt(3.0) * x, (rows == nin).astype(jnp.float32))
    q2 = math.sqrt(5.0) * (1.5 * x * x - 0.5) * root
    q3 = math.sqrt(7.0) * (2.5 * x * x * x - 1.5 * x) * root
    parts = [q1 * root, q2[0:nin, :], q3[0:nin, :]]
    spare = plan.rows_a - plan.q3 - nin
    if spare:
        parts.append(jnp.zeros((spare, x.shape[1]), jnp.float32))
    ta[0 : plan.rows_a, :], ta[plan.rows_a : 2 * plan.rows_a, :] = split(jnp.concatenate(parts, axis=0))
    work[0:single, :] = q1
    for begin, end, base in ((0, plan.half, plan.low), (plan.half, nin, plan.high)):
        for b in range(1, end - begin):
            at = base + b * (b - 1) // 2
            work[at : at + b, :] = q1[begin : begin + b, :] * q1[begin + b : begin + b + 1, :]
    tb[0 : plan.rows_b, :], tb[plan.rows_b : 2 * plan.rows_b, :] = split(work[...])


def xor_index(a, b, n):
    if n & (n - 1):
        return lax.rem(a + b, n)
    out, bit = 0, 1
    while bit < n:
        out = out + bit * (((a // bit) % 2 + (b // bit) % 2) % 2)
        bit *= 2
    return out


def kernel(
    plan, sizes, columns, samples_total,
    x_hbm, w_hbm, y_hbm, deg_hbm, acc,
    slabs, x_ref, w_ref, y_ref, deg_ref, codes_in, sel_a, sel_b, ta0, tb0, z0, ta1, tb1, z1, work0, work1, d0, d1,
    load_sem, ici_send, sub_send, recv, code_send, code_recv,
):
    nsmp, nsub, ntrm = sizes
    smp, sub, trm = lax.axis_index("smp"), lax.axis_index("sub"), lax.axis_index("trm")
    me = smp * nsub + sub
    nin = plan.nin
    terms = deg_ref.shape[1]
    width = codes_in.shape[2]
    right = up(columns, 16)

    barrier = pltpu.get_barrier_semaphore()
    for d in range(1, nsmp):
        pl.semaphore_signal(barrier, inc=1, device_id={"smp": xor_index(smp, d, nsmp)}, device_id_type=MESH)
    for d in range(1, nsub):
        pl.semaphore_signal(barrier, inc=1, device_id={"sub": lax.rem(sub + d, nsub)}, device_id_type=MESH)
    for d in range(1, ntrm):
        pl.semaphore_signal(barrier, inc=1, device_id={"trm": lax.rem(trm + d, ntrm)}, device_id_type=MESH)

    mine = slabs.at[me]
    loads = [
        pltpu.make_async_copy(deg_hbm, deg_ref, load_sem.at[0]),
        pltpu.make_async_copy(x_hbm, x_ref, load_sem.at[1]),
        pltpu.make_async_copy(w_hbm, w_ref, load_sem.at[2]),
        pltpu.make_async_copy(y_hbm, y_ref, load_sem.at[3]),
    ]
    for load in loads:
        load.start()
    work0[...] = jnp.zeros_like(work0)
    work1[...] = jnp.zeros_like(work1)
    acc[...] = jnp.zeros_like(acc)
    for load in loads[1:]:
        load.wait()
    spare = plan.slab - nin - 2
    mine[...] = jnp.concatenate(
        [x_ref[...], w_ref[...], y_ref[...], jnp.zeros((spare, x_ref.shape[1]), jnp.float32)], axis=0
    )
    loads[0].wait()
    code = positions(plan, deg_ref[...])
    per_trm = terms // columns
    for k in range(per_trm):
        @pl.when(lax.rem(me, per_trm) == k)
        def _():
            part = code[:, k * columns : (k + 1) * columns].astype(jnp.float32)
            pad = jnp.full((1, width - columns), -1.0, jnp.float32)
            codes_in[trm] = jnp.broadcast_to(jnp.concatenate([part, pad], axis=1), (8, width))

    pl.semaphore_wait(barrier, (nsmp - 1) + (nsub - 1) + (ntrm - 1))

    def sub_copy(chunk, p, d):
        return pltpu.make_async_remote_copy(
            src_ref=slabs.at[chunk], dst_ref=slabs.at[chunk],
            send_sem=sub_send.at[p, d - 1], recv_sem=recv.at[chunk],
            device_id={"sub": lax.rem(sub + d, nsub)}, device_id_type=MESH,
        )

    def ici_copy(d):
        return pltpu.make_async_remote_copy(
            src_ref=slabs.at[me], dst_ref=slabs.at[me],
            send_sem=ici_send.at[d - 1], recv_sem=recv.at[me],
            device_id={"smp": xor_index(smp, d, nsmp)}, device_id_type=MESH,
        )

    def code_copy(d):
        return pltpu.make_async_remote_copy(
            src_ref=codes_in.at[trm], dst_ref=codes_in.at[trm],
            send_sem=code_send.at[d - 1], recv_sem=code_recv.at[trm],
            device_id={"trm": lax.rem(trm + d, ntrm)}, device_id_type=MESH,
        )

    def wait_slab(chunk):
        pltpu.make_async_remote_copy(
            src_ref=slabs.at[chunk], dst_ref=slabs.at[chunk],
            send_sem=ici_send.at[0], recv_sem=recv.at[chunk],
            device_id={"sub": lax.rem(sub + 1, nsub)}, device_id_type=MESH,
        ).wait_recv()

    for d in range(1, nsmp):
        ici_copy(d).start()
    for d in range(1, nsub):
        sub_copy(me, 0, d).start()
    for d in range(1, ntrm):
        code_copy(d).start()

    build_tables(plan, samples_total, slabs[me], work0, ta0, tb0, z0)

    def select(row, base, count, limit):
        column = jnp.broadcast_to(row, (128, 128)).T.astype(jnp.int32)[0:count, :]
        for ref, wanted, rows in ((sel_a, column >> 8, plan.rows_a), (sel_b, column & (BASE - 1), plan.rows_b)):
            for j in range(0, ref.shape[1], 128):
                lane = lax.rem(lax.broadcasted_iota(jnp.int32, (count, 128), 1) + j, rows)
                ref[base : base + count, j : j + 128] = (wanted == lane).astype(jnp.bfloat16)

    for i in range(0, terms, 128):
        count = min(128, terms - i)
        row = code[:, i : i + count].astype(jnp.float32)
        if count < 128:
            row = jnp.concatenate([row, jnp.zeros((1, 128 - count), jnp.float32)], axis=1)
        select(row, i, count, terms)

    for d in range(1, ntrm):
        other = lax.rem(trm + d, ntrm)
        pltpu.make_async_remote_copy(
            src_ref=codes_in.at[other], dst_ref=codes_in.at[other],
            send_sem=code_send.at[d - 1], recv_sem=code_recv.at[other],
            device_id={"trm": other}, device_id_type=MESH,
        ).wait_recv()
    wanted = codes_in[me // per_trm]
    for i in range(0, right, 128):
        select(wanted[0:1, i : i + 128], terms + i, min(128, right - i), right)

    def chunk_of(p, s):
        return xor_index(smp, p, nsmp) * nsub + lax.rem(sub + s, nsub)

    def compute(ta, tb, z_ref, d_ref):
        dims = (((1,), (0,)), ((), ()))
        selected = terms + right
        for n in range(0, d_ref.shape[1], 256):
            a = lax.dot_general(sel_a[...], ta[:, n : n + 256], dims, preferred_element_type=jnp.float32)
            b = lax.dot_general(sel_b[...], tb[:, n : n + 256], dims, preferred_element_type=jnp.float32)
            d_ref[0:selected, n : n + 256] = (a * b).astype(jnp.bfloat16)
        d_ref[selected : selected + 16, :] = z_ref[...]
        for c in range(0, terms, 256):
            e = min(c + 256, terms)
            acc[:, c:e] += lax.dot_general(
                d_ref[terms : selected + 16, :], d_ref[c:e, :], (((1,), (1,)), ((), ())),
                preferred_element_type=jnp.float32,
            )

    def body(p, carry):
        second = chunk_of(p, 1)
        wait_slab(second)
        compute(ta0, tb0, z0, d0)
        build_tables(plan, samples_total, slabs[second], work1, ta1, tb1, z1)
        following = chunk_of(lax.rem(p + 1, nsmp), 0)

        @pl.when(p + 1 < nsmp)
        def _():
            wait_slab(following)
            for d in range(1, nsub):
                sub_copy(following, p + 1, d).start()

        compute(ta1, tb1, z1, d1)
        build_tables(plan, samples_total, slabs[following], work0, ta0, tb0, z0)
        return carry

    lax.fori_loop(0, nsmp, body, 0)

    for d in range(1, ntrm):
        code_copy(d).wait_send()
    for d in range(1, nsmp):
        ici_copy(d).wait_send()
    for p in range(nsmp):
        for d in range(1, nsub):
            sub_copy(chunk_of(p, 0), p, d).wait_send()


def write_out(columns, acc_ref, gram_out, rhs_out, flat, sem):
    copy = pltpu.make_async_copy(acc_ref.at[0 : gram_out.shape[0], :], gram_out, sem.at[0])
    copy.start()
    z = up(columns, 16)
    terms = acc_ref.shape[1]
    line = acc_ref[z : z + 1, :] + acc_ref[z + 1 : z + 2, :]
    line = jnp.concatenate([line, jnp.zeros((1, flat.shape[0] - terms), jnp.float32)], axis=1)
    rows = [line[:, i : i + 128] for i in range(0, flat.shape[0], 128)]
    flat[...] = jnp.concatenate(rows, axis=0).reshape(flat.shape)
    tail = pltpu.make_async_copy(flat.at[pl.ds(0, rhs_out.shape[0])], rhs_out, sem.at[1])
    tail.start()
    tail.wait()
    copy.wait()


def solution(mesh):
    nsmp, nsub, ntrm = mesh.shape["smp"], mesh.shape["sub"], mesh.shape["trm"]

    def local(inputs, weights, response, index_table):
        nin, samples = inputs.shape
        terms = index_table.shape[1]
        columns = terms * ntrm // (nsmp * nsub)
        plan = Plan(nin)
        right = up(columns, 16)
        width = up(columns, 128)
        chunks = nsmp * nsub
        acc = pl.pallas_call(
            functools.partial(kernel, plan, (nsmp, nsub, ntrm), columns, samples * chunks),
            out_shape=pltpu.VMEM((right + 16, terms), jnp.float32),
            in_specs=[pl.BlockSpec(memory_space=pltpu.HBM)] * 4,
            out_specs=pl.BlockSpec(memory_space=pltpu.VMEM),
            scratch_shapes=[
                pltpu.VMEM((chunks, plan.slab, samples), jnp.float32),
                pltpu.VMEM((nin, samples), jnp.float32),
                pltpu.VMEM((1, samples), jnp.float32),
                pltpu.VMEM((1, samples), jnp.float32),
                pltpu.VMEM((nin, terms), jnp.int32),
                pltpu.VMEM((ntrm, 8, width), jnp.float32),
                pltpu.VMEM((terms + right, 2 * plan.rows_a), jnp.bfloat16),
                pltpu.VMEM((terms + right, 2 * plan.rows_b), jnp.bfloat16),
            ]
            + [
                pltpu.VMEM((2 * plan.rows_a, samples), jnp.bfloat16),
                pltpu.VMEM((2 * plan.rows_b, samples), jnp.bfloat16),
                pltpu.VMEM((16, samples), jnp.bfloat16),
            ]
            * 2
            + [pltpu.VMEM((plan.rows_b, samples), jnp.float32)] * 2
            + [pltpu.VMEM((terms + right + 16, samples), jnp.bfloat16)] * 2
            + [
                pltpu.SemaphoreType.DMA((4,)),
                pltpu.SemaphoreType.DMA((max(nsmp - 1, 1),)),
                pltpu.SemaphoreType.DMA((nsmp, max(nsub - 1, 1))),
                pltpu.SemaphoreType.DMA((chunks,)),
                pltpu.SemaphoreType.DMA((max(ntrm - 1, 1),)),
                pltpu.SemaphoreType.DMA((ntrm,)),
            ],
            compiler_params=pltpu.CompilerParams(
                collective_id=0, has_side_effects=True, vmem_limit_bytes=40 * 1024 * 1024
            ),
        )(*map(
            lambda v: pltpu.with_memory_space_constraint(v, pltpu.HBM),
            (inputs, weights.reshape(1, samples), response.reshape(1, samples), index_table),
        ))
        gram, rhs = pl.pallas_call(
            functools.partial(write_out, columns),
            out_shape=(
                jax.ShapeDtypeStruct((up(columns, 8), terms), jnp.float32),
                jax.ShapeDtypeStruct((up(terms, 1024) if terms % 128 else terms,), jnp.float32),
            ),
            in_specs=[pl.BlockSpec(memory_space=pltpu.VMEM)],
            out_specs=(pl.BlockSpec(memory_space=pl.ANY),) * 2,
            scratch_shapes=[
                pltpu.VMEM((up(terms, 1024),), jnp.float32),
                pltpu.SemaphoreType.DMA((2,)),
            ],
        )(pltpu.with_memory_space_constraint(acc, pltpu.VMEM))
        return gram[0:columns].T, rhs[0:terms]

    return jax.shard_map(
        local,
        mesh=mesh,
        in_specs=(
            P(None, ("grp", "smp", "sub")),
            P(("grp", "smp", "sub")),
            P(("grp", "smp", "sub")),
            P(None, "trm"),
        ),
        out_specs=(P(("grp", "trm"), ("smp", "sub")), P(("grp", "trm"))),
        check_vma=False,
    )
```

```python
import functools
import math

import jax
import jax.numpy as jnp
from jax import lax
from jax.experimental import pallas as pl
from jax.experimental.pallas import tpu as pltpu
from jax.sharding import PartitionSpec as P

MESH = pl.DeviceIdType.MESH
BASE = 256


def up(n, m):
    return -(-n // m) * m


class Plan:
    def __init__(self, nin):
        self.nin = nin
        self.half = nin // 2
        self.single = up(nin + 1, 8)
        self.slab = up(nin + 2, 8)
        self.q2 = self.single
        self.q3 = self.single + nin
        self.rows_a = max(up(self.single + 2 * nin, 16), 64)
        self.low = self.single
        self.high = self.low + self.half * (self.half - 1) // 2
        rest = nin - self.half
        self.rows_b = max(up(self.high + rest * (rest - 1) // 2, 16), 128)


def positions(plan, degrees):
    degrees = degrees.astype(jnp.float32)
    index = lax.broadcasted_iota(jnp.int32, degrees.shape, 0).astype(jnp.float32)
    present = degrees > 0
    total = jnp.sum(degrees, axis=0, keepdims=True)
    weighted = jnp.sum(degrees * index, axis=0, keepdims=True).astype(jnp.int32)
    least = jnp.min(jnp.where(present, index, plan.nin), axis=0, keepdims=True).astype(jnp.int32)
    most = jnp.max(jnp.where(present, index, -1), axis=0, keepdims=True).astype(jnp.int32)
    first = least
    second = jnp.where(total > 2, weighted - least - most, jnp.where(total > 1, most, plan.nin))
    third = jnp.where(total > 2, most, plan.nin)
    nin, half = plan.nin, plan.half
    low = second < half
    big = jnp.where(low, second, third - half)
    small = jnp.where(low, first, second - half)
    pair = jnp.where(low, plan.low, plan.high) + (big * (big - 1)) // 2 + small
    a = jnp.where(low, third, first)
    b = pair
    twin = (first == second) | (second == third)
    a = jnp.where(twin, plan.q2 + second, a)
    b = jnp.where(twin, jnp.where(first == second, third, first), b)
    triple = (first == second) & (second == third)
    a = jnp.where(triple, plan.q3 + first, a)
    b = jnp.where(triple, nin, b)
    a = jnp.where((third == nin) & (first != second), first, a)
    b = jnp.where((third == nin) & (first != second), second, b)
    a = jnp.where(first == nin, nin, a)
    b = jnp.where(first == nin, nin, b)
    return a * BASE + b


def split(v):
    high = v.astype(jnp.bfloat16)
    return high, (v - high.astype(jnp.float32)).astype(jnp.bfloat16)


def build_tables(plan, samples_total, slab, work, ta, tb, z_ref):
    nin, single = plan.nin, plan.single
    x = slab[0:single, :]
    weights = slab[nin : nin + 1, :]
    root = jnp.sqrt(weights / samples_total)
    scaled = weights * slab[nin + 1 : nin + 2, :] / samples_total
    z_high, z_low = split(scaled.astype(jnp.bfloat16).astype(jnp.float32) / root)
    z_ref[...] = jnp.concatenate(
        [z_high.astype(jnp.float32), z_low.astype(jnp.float32), jnp.zeros((14, x.shape[1]), jnp.float32)], axis=0
    ).astype(jnp.bfloat16)
    rows = lax.broadcasted_iota(jnp.int32, x.shape, 0)
    q1 = jnp.where(rows < nin, math.sqrt(3.0) * x, (rows == nin).astype(jnp.float32))
    q2 = math.sqrt(5.0) * (1.5 * x * x - 0.5) * root
    q3 = math.sqrt(7.0) * (2.5 * x * x * x - 1.5 * x) * root
    parts = [q1 * root, q2[0:nin, :], q3[0:nin, :]]
    spare = plan.rows_a - plan.q3 - nin
    if spare:
        parts.append(jnp.zeros((spare, x.shape[1]), jnp.float32))
    ta[0 : plan.rows_a, :], ta[plan.rows_a : 2 * plan.rows_a, :] = split(jnp.concatenate(parts, axis=0))
    work[0:single, :] = q1
    for begin, end, base in ((0, plan.half, plan.low), (plan.half, nin, plan.high)):
        for b in range(1, end - begin):
            at = base + b * (b - 1) // 2
            work[at : at + b, :] = q1[begin : begin + b, :] * q1[begin + b : begin + b + 1, :]
    tb[0 : plan.rows_b, :], tb[plan.rows_b : 2 * plan.rows_b, :] = split(work[...])


def xor_index(a, b, n):
    if n & (n - 1):
        return lax.rem(a + b, n)
    out, bit = 0, 1
    while bit < n:
        out = out + bit * (((a // bit) % 2 + (b // bit) % 2) % 2)
        bit *= 2
    return out


def kernel(
    plan, sizes, columns, samples_total,
    x_hbm, w_hbm, y_hbm, deg_hbm, acc,
    slabs, x_ref, w_ref, y_ref, deg_ref, codes_in, sel_a, sel_b, ta0, tb0, z0, ta1, tb1, z1, work0, work1, d0, d1,
    load_sem, ici_send, sub_send, recv, code_send, code_recv,
):
    nsmp, nsub, ntrm = sizes
    smp, sub, trm = lax.axis_index("smp"), lax.axis_index("sub"), lax.axis_index("trm")
    me = smp * nsub + sub
    nin = plan.nin
    terms = deg_ref.shape[1]
    width = codes_in.shape[2]
    right = up(columns, 16)
    selected = terms + right

    barrier = pltpu.get_barrier_semaphore()
    for d in range(1, nsmp):
        pl.semaphore_signal(barrier, inc=1, device_id={"smp": xor_index(smp, d, nsmp)}, device_id_type=MESH)
    for d in range(1, nsub):
        pl.semaphore_signal(barrier, inc=1, device_id={"sub": lax.rem(sub + d, nsub)}, device_id_type=MESH)
    for d in range(1, ntrm):
        pl.semaphore_signal(barrier, inc=1, device_id={"trm": lax.rem(trm + d, ntrm)}, device_id_type=MESH)

    mine = slabs.at[me]
    loads = [
        pltpu.make_async_copy(deg_hbm, deg_ref, load_sem.at[0]),
        pltpu.make_async_copy(x_hbm, x_ref, load_sem.at[1]),
        pltpu.make_async_copy(w_hbm, w_ref, load_sem.at[2]),
        pltpu.make_async_copy(y_hbm, y_ref, load_sem.at[3]),
    ]
    for load in loads:
        load.start()
    work0[...] = jnp.zeros_like(work0)
    work1[...] = jnp.zeros_like(work1)
    acc[...] = jnp.zeros_like(acc)
    for load in loads[1:]:
        load.wait()
    spare = plan.slab - nin - 2
    mine[...] = jnp.concatenate(
        [x_ref[...], w_ref[...], y_ref[...], jnp.zeros((spare, x_ref.shape[1]), jnp.float32)], axis=0
    )
    loads[0].wait()
    code = positions(plan, deg_ref[...])
    per_trm = terms // columns
    for k in range(per_trm):
        @pl.when(lax.rem(me, per_trm) == k)
        def _():
            part = code[:, k * columns : (k + 1) * columns].astype(jnp.float32)
            pad = jnp.full((1, width - columns), -1.0, jnp.float32)
            codes_in[trm] = jnp.broadcast_to(jnp.concatenate([part, pad], axis=1), (8, width))

    pl.semaphore_wait(barrier, (nsmp - 1) + (nsub - 1) + (ntrm - 1))

    def sub_copy(chunk, p, d):
        return pltpu.make_async_remote_copy(
            src_ref=slabs.at[chunk], dst_ref=slabs.at[chunk],
            send_sem=sub_send.at[p, d - 1], recv_sem=recv.at[chunk],
            device_id={"sub": lax.rem(sub + d, nsub)}, device_id_type=MESH,
        )

    def ici_copy(d):
        return pltpu.make_async_remote_copy(
            src_ref=slabs.at[me], dst_ref=slabs.at[me],
            send_sem=ici_send.at[d - 1], recv_sem=recv.at[me],
            device_id={"smp": xor_index(smp, d, nsmp)}, device_id_type=MESH,
        )

    def code_copy(d):
        return pltpu.make_async_remote_copy(
            src_ref=codes_in.at[trm], dst_ref=codes_in.at[trm],
            send_sem=code_send.at[d - 1], recv_sem=code_recv.at[trm],
            device_id={"trm": lax.rem(trm + d, ntrm)}, device_id_type=MESH,
        )

    def wait_slab(chunk):
        pltpu.make_async_remote_copy(
            src_ref=slabs.at[chunk], dst_ref=slabs.at[chunk],
            send_sem=ici_send.at[0], recv_sem=recv.at[chunk],
            device_id={"sub": lax.rem(sub + 1, nsub)}, device_id_type=MESH,
        ).wait_recv()

    for d in range(1, nsmp):
        ici_copy(d).start()
    for d in range(1, nsub):
        sub_copy(me, 0, d).start()
    for d in range(1, ntrm):
        code_copy(d).start()

    def chunk_of(p, s):
        return xor_index(smp, p, nsmp) * nsub + lax.rem(sub + s, nsub)

    def pick(ta, tb, d_ref, begin, end):
        dims = (((1,), (0,)), ((), ()))
        for n in range(0, d_ref.shape[1], 256):
            a = lax.dot_general(sel_a[begin:end, :], ta[:, n : n + 256], dims, preferred_element_type=jnp.float32)
            b = lax.dot_general(sel_b[begin:end, :], tb[:, n : n + 256], dims, preferred_element_type=jnp.float32)
            d_ref[begin:end, n : n + 256] = (a * b).astype(jnp.bfloat16)

    def add(z_ref, d_ref):
        d_ref[selected : selected + 16, :] = z_ref[...]
        for c in range(0, terms, 256):
            e = min(c + 256, terms)
            acc[:, c:e] += lax.dot_general(
                d_ref[terms : selected + 16, :], d_ref[c:e, :], (((1,), (1,)), ((), ())),
                preferred_element_type=jnp.float32,
            )

    def next_own(p):
        following = chunk_of(lax.rem(p + 1, nsmp), 0)

        @pl.when(p + 1 < nsmp)
        def _():
            wait_slab(following)
            for d in range(1, nsub):
                sub_copy(following, p + 1, d).start()

        return slabs[following]

    set0, set1 = (work0, ta0, tb0, z0), (work1, ta1, tb1, z1)

    build_tables(plan, samples_total, slabs[me], *set0)

    def select(row, base, count):
        column = jnp.broadcast_to(row, (128, 128)).T.astype(jnp.int32)[0:count, :]
        for ref, wanted, rows in ((sel_a, column >> 8, plan.rows_a), (sel_b, column & (BASE - 1), plan.rows_b)):
            for j in range(0, ref.shape[1], 128):
                lane = lax.rem(lax.broadcasted_iota(jnp.int32, (count, 128), 1) + j, rows)
                ref[base : base + count, j : j + 128] = (wanted == lane).astype(jnp.bfloat16)

    for i in range(0, terms, 128):
        count = min(128, terms - i)
        row = code[:, i : i + count].astype(jnp.float32)
        if count < 128:
            row = jnp.concatenate([row, jnp.zeros((1, 128 - count), jnp.float32)], axis=1)
        select(row, i, count)

    partner = chunk_of(0, 1)
    pick(ta0, tb0, d0, 0, terms)
    wait_slab(partner)
    build_tables(plan, samples_total, slabs[partner], *set1)
    pick(ta1, tb1, d1, 0, terms)

    for d in range(1, ntrm):
        other = lax.rem(trm + d, ntrm)
        pltpu.make_async_remote_copy(
            src_ref=codes_in.at[other], dst_ref=codes_in.at[other],
            send_sem=code_send.at[d - 1], recv_sem=code_recv.at[other],
            device_id={"trm": other}, device_id_type=MESH,
        ).wait_recv()
    wanted = codes_in[me // per_trm]
    for i in range(0, right, 128):
        select(wanted[0:1, i : i + 128], terms + i, min(128, right - i))
    pick(ta0, tb0, d0, terms, selected)

    add(z0, d0)
    following = next_own(0)
    pick(ta1, tb1, d1, terms, selected)
    add(z1, d1)
    build_tables(plan, samples_total, following, *set0)

    def body(p, carry):
        second = chunk_of(p, 1)
        wait_slab(second)
        pick(ta0, tb0, d0, 0, selected)
        add(z0, d0)
        build_tables(plan, samples_total, slabs[second], *set1)
        following = next_own(p)
        pick(ta1, tb1, d1, 0, selected)
        add(z1, d1)
        build_tables(plan, samples_total, following, *set0)
        return carry

    lax.fori_loop(1, nsmp, body, 0)

    for d in range(1, ntrm):
        code_copy(d).wait_send()
    for d in range(1, nsmp):
        ici_copy(d).wait_send()
    for p in range(nsmp):
        for d in range(1, nsub):
            sub_copy(chunk_of(p, 0), p, d).wait_send()


def write_out(columns, acc_ref, gram_out, rhs_out, flat, sem):
    copy = pltpu.make_async_copy(acc_ref.at[0 : gram_out.shape[0], :], gram_out, sem.at[0])
    copy.start()
    z = up(columns, 16)
    terms = acc_ref.shape[1]
    line = acc_ref[z : z + 1, :] + acc_ref[z + 1 : z + 2, :]
    line = jnp.concatenate([line, jnp.zeros((1, flat.shape[0] - terms), jnp.float32)], axis=1)
    rows = [line[:, i : i + 128] for i in range(0, flat.shape[0], 128)]
    flat[...] = jnp.concatenate(rows, axis=0).reshape(flat.shape)
    tail = pltpu.make_async_copy(flat.at[pl.ds(0, rhs_out.shape[0])], rhs_out, sem.at[1])
    tail.start()
    tail.wait()
    copy.wait()


def solution(mesh):
    nsmp, nsub, ntrm = mesh.shape["smp"], mesh.shape["sub"], mesh.shape["trm"]

    def local(inputs, weights, response, index_table):
        nin, samples = inputs.shape
        terms = index_table.shape[1]
        columns = terms * ntrm // (nsmp * nsub)
        plan = Plan(nin)
        right = up(columns, 16)
        width = up(columns, 128)
        chunks = nsmp * nsub
        acc = pl.pallas_call(
            functools.partial(kernel, plan, (nsmp, nsub, ntrm), columns, samples * chunks),
            out_shape=pltpu.VMEM((right + 16, terms), jnp.float32),
            in_specs=[pl.BlockSpec(memory_space=pltpu.HBM)] * 4,
            out_specs=pl.BlockSpec(memory_space=pltpu.VMEM),
            scratch_shapes=[
                pltpu.VMEM((chunks, plan.slab, samples), jnp.float32),
                pltpu.VMEM((nin, samples), jnp.float32),
                pltpu.VMEM((1, samples), jnp.float32),
                pltpu.VMEM((1, samples), jnp.float32),
                pltpu.VMEM((nin, terms), jnp.int32),
                pltpu.VMEM((ntrm, 8, width), jnp.float32),
                pltpu.VMEM((terms + right, 2 * plan.rows_a), jnp.bfloat16),
                pltpu.VMEM((terms + right, 2 * plan.rows_b), jnp.bfloat16),
            ]
            + [
                pltpu.VMEM((2 * plan.rows_a, samples), jnp.bfloat16),
                pltpu.VMEM((2 * plan.rows_b, samples), jnp.bfloat16),
                pltpu.VMEM((16, samples), jnp.bfloat16),
            ]
            * 2
            + [pltpu.VMEM((plan.rows_b, samples), jnp.float32)] * 2
            + [pltpu.VMEM((terms + right + 16, samples), jnp.bfloat16)] * 2
            + [
                pltpu.SemaphoreType.DMA((4,)),
                pltpu.SemaphoreType.DMA((max(nsmp - 1, 1),)),
                pltpu.SemaphoreType.DMA((nsmp, max(nsub - 1, 1))),
                pltpu.SemaphoreType.DMA((chunks,)),
                pltpu.SemaphoreType.DMA((max(ntrm - 1, 1),)),
                pltpu.SemaphoreType.DMA((ntrm,)),
            ],
            compiler_params=pltpu.CompilerParams(
                collective_id=0, has_side_effects=True, vmem_limit_bytes=40 * 1024 * 1024
            ),
        )(*map(
            lambda v: pltpu.with_memory_space_constraint(v, pltpu.HBM),
            (inputs, weights.reshape(1, samples), response.reshape(1, samples), index_table),
        ))
        gram, rhs = pl.pallas_call(
            functools.partial(write_out, columns),
            out_shape=(
                jax.ShapeDtypeStruct((up(columns, 8), terms), jnp.float32),
                jax.ShapeDtypeStruct((up(terms, 1024) if terms % 128 else terms,), jnp.float32),
            ),
            in_specs=[pl.BlockSpec(memory_space=pltpu.VMEM)],
            out_specs=(pl.BlockSpec(memory_space=pl.ANY),) * 2,
            scratch_shapes=[
                pltpu.VMEM((up(terms, 1024),), jnp.float32),
                pltpu.SemaphoreType.DMA((2,)),
            ],
        )(pltpu.with_memory_space_constraint(acc, pltpu.VMEM))
        return gram[0:columns].T, rhs[0:terms]

    return jax.shard_map(
        local,
        mesh=mesh,
        in_specs=(
            P(None, ("grp", "smp", "sub")),
            P(("grp", "smp", "sub")),
            P(("grp", "smp", "sub")),
            P(None, "trm"),
        ),
        out_specs=(P(("grp", "trm"), ("smp", "sub")), P(("grp", "trm"))),
        check_vma=False,
    )
```

```python
import functools
import math

import jax
import jax.numpy as jnp
from jax import lax
from jax.experimental import pallas as pl
from jax.experimental.pallas import tpu as pltpu
from jax.sharding import PartitionSpec as P

MESH = pl.DeviceIdType.MESH
BASE = 256
SCALE_X = 32767.0
SCALE_W = 8191.0


def up(n, m):
    return -(-n // m) * m


class Plan:
    def __init__(self, nin):
        self.nin = nin
        self.half = nin // 2
        self.single = up(nin + 1, 8)
        self.groups = -(-(nin + 4) // 8)
        self.q2 = self.single
        self.q3 = self.single + nin
        self.rows_a = max(up(self.single + 2 * nin, 16), 64)
        self.low = self.single
        self.high = self.low + self.half * (self.half - 1) // 2
        rest = nin - self.half
        self.rows_b = max(up(self.high + rest * (rest - 1) // 2, 16), 128)


def positions(plan, degrees):
    degrees = degrees.astype(jnp.float32)
    index = lax.broadcasted_iota(jnp.int32, degrees.shape, 0).astype(jnp.float32)
    present = degrees > 0
    total = jnp.sum(degrees, axis=0, keepdims=True)
    weighted = jnp.sum(degrees * index, axis=0, keepdims=True).astype(jnp.int32)
    least = jnp.min(jnp.where(present, index, plan.nin), axis=0, keepdims=True).astype(jnp.int32)
    most = jnp.max(jnp.where(present, index, -1), axis=0, keepdims=True).astype(jnp.int32)
    first = least
    second = jnp.where(total > 2, weighted - least - most, jnp.where(total > 1, most, plan.nin))
    third = jnp.where(total > 2, most, plan.nin)
    nin, half = plan.nin, plan.half
    low = second < half
    big = jnp.where(low, second, third - half)
    small = jnp.where(low, first, second - half)
    pair = jnp.where(low, plan.low, plan.high) + (big * (big - 1)) // 2 + small
    a = jnp.where(low, third, first)
    b = pair
    twin = (first == second) | (second == third)
    a = jnp.where(twin, plan.q2 + second, a)
    b = jnp.where(twin, jnp.where(first == second, third, first), b)
    triple = (first == second) & (second == third)
    a = jnp.where(triple, plan.q3 + first, a)
    b = jnp.where(triple, nin, b)
    a = jnp.where((third == nin) & (first != second), first, a)
    b = jnp.where((third == nin) & (first != second), second, b)
    a = jnp.where(first == nin, nin, a)
    b = jnp.where(first == nin, nin, b)
    return a * BASE + b


def split(v):
    high = v.astype(jnp.bfloat16)
    return high, (v - high.astype(jnp.float32)).astype(jnp.bfloat16)


def coarse_fine(v):
    v = v * SCALE_W
    coarse = jnp.round(v)
    return [coarse, jnp.round((v - coarse) * (2.0 * SCALE_X))]


def encode(plan, x, weights, response):
    rows = [jnp.round(x * SCALE_X)] + coarse_fine(weights) + coarse_fine(response)
    spare = 8 * plan.groups - plan.nin - 4
    if spare:
        rows.append(jnp.zeros((spare, x.shape[1]), jnp.float32))
    rows = jnp.concatenate(rows, axis=0).astype(jnp.int32)
    half = x.shape[1] // 2
    parts = []
    for g in range(plan.groups):
        group = rows[8 * g : 8 * g + 8, :]
        parts.append(jnp.concatenate([group[:, 0:half], group[:, half:]], axis=0))
    return jnp.concatenate(parts, axis=1).astype(jnp.int16)


def decode(plan, slab):
    half = slab.shape[1] // plan.groups
    parts = []
    for g in range(plan.groups):
        group = slab[:, g * half : (g + 1) * half].astype(jnp.int32).astype(jnp.float32)
        parts.append(jnp.concatenate([group[0:8, :], group[8:16, :]], axis=1))
    return jnp.concatenate(parts, axis=0)


def build_tables(plan, samples_total, slab, work, ta, tb, z_ref):
    nin, single = plan.nin, plan.single
    rows = decode(plan, slab)

    def joined(i):
        return (rows[i : i + 1, :] + rows[i + 1 : i + 2, :] * (0.5 / SCALE_X)) * (1.0 / SCALE_W)

    x = rows[0:single, :] * (1.0 / SCALE_X)
    weights = joined(nin)
    root = jnp.sqrt(weights / samples_total)
    scaled = weights * joined(nin + 2) / samples_total
    z_high, z_low = split(scaled.astype(jnp.bfloat16).astype(jnp.float32) / root)
    z_ref[...] = jnp.concatenate(
        [z_high.astype(jnp.float32), z_low.astype(jnp.float32), jnp.zeros((14, x.shape[1]), jnp.float32)], axis=0
    ).astype(jnp.bfloat16)
    index = lax.broadcasted_iota(jnp.int32, x.shape, 0)
    q1 = jnp.where(index < nin, math.sqrt(3.0) * x, (index == nin).astype(jnp.float32))
    q2 = math.sqrt(5.0) * (1.5 * x * x - 0.5) * root
    q3 = math.sqrt(7.0) * (2.5 * x * x * x - 1.5 * x) * root
    parts = [q1 * root, q2[0:nin, :], q3[0:nin, :]]
    spare = plan.rows_a - plan.q3 - nin
    if spare:
        parts.append(jnp.zeros((spare, x.shape[1]), jnp.float32))
    ta[0 : plan.rows_a, :], ta[plan.rows_a : 2 * plan.rows_a, :] = split(jnp.concatenate(parts, axis=0))
    work[0:single, :] = q1
    for begin, end, base in ((0, plan.half, plan.low), (plan.half, nin, plan.high)):
        for b in range(1, end - begin):
            at = base + b * (b - 1) // 2
            work[at : at + b, :] = q1[begin : begin + b, :] * q1[begin + b : begin + b + 1, :]
    tb[0 : plan.rows_b, :], tb[plan.rows_b : 2 * plan.rows_b, :] = split(work[...])


def xor_index(a, b, n):
    if n & (n - 1):
        return lax.rem(a + b, n)
    out, bit = 0, 1
    while bit < n:
        out = out + bit * (((a // bit) % 2 + (b // bit) % 2) % 2)
        bit *= 2
    return out


def kernel(
    plan, sizes, columns, samples_total,
    x_hbm, w_hbm, y_hbm, deg_hbm, acc,
    slabs, x_ref, w_ref, y_ref, deg_ref, codes_in, sel_a, sel_b, ta0, tb0, z0, ta1, tb1, z1, work0, work1, d0, d1,
    load_sem, ici_send, sub_send, recv, code_send, code_recv,
):
    nsmp, nsub, ntrm = sizes
    smp, sub, trm = lax.axis_index("smp"), lax.axis_index("sub"), lax.axis_index("trm")
    me = smp * nsub + sub
    nin = plan.nin
    terms = deg_ref.shape[1]
    width = codes_in.shape[2]
    right = up(columns, 16)
    selected = terms + right

    barrier = pltpu.get_barrier_semaphore()
    for d in range(1, nsmp):
        pl.semaphore_signal(barrier, inc=1, device_id={"smp": xor_index(smp, d, nsmp)}, device_id_type=MESH)
    for d in range(1, nsub):
        pl.semaphore_signal(barrier, inc=1, device_id={"sub": lax.rem(sub + d, nsub)}, device_id_type=MESH)
    for d in range(1, ntrm):
        pl.semaphore_signal(barrier, inc=1, device_id={"trm": lax.rem(trm + d, ntrm)}, device_id_type=MESH)

    mine = slabs.at[me]
    loads = [
        pltpu.make_async_copy(deg_hbm, deg_ref, load_sem.at[0]),
        pltpu.make_async_copy(x_hbm, x_ref, load_sem.at[1]),
        pltpu.make_async_copy(w_hbm, w_ref, load_sem.at[2]),
        pltpu.make_async_copy(y_hbm, y_ref, load_sem.at[3]),
    ]
    for load in loads:
        load.start()
    work0[...] = jnp.zeros_like(work0)
    work1[...] = jnp.zeros_like(work1)
    acc[...] = jnp.zeros_like(acc)
    for load in loads[1:]:
        load.wait()
    mine[...] = encode(plan, x_ref[...], w_ref[...], y_ref[...])
    loads[0].wait()
    code = positions(plan, deg_ref[...])
    per_trm = terms // columns
    for k in range(per_trm):
        @pl.when(lax.rem(me, per_trm) == k)
        def _():
            part = code[:, k * columns : (k + 1) * columns].astype(jnp.float32)
            pad = jnp.full((1, width - columns), -1.0, jnp.float32)
            codes_in[trm] = jnp.broadcast_to(jnp.concatenate([part, pad], axis=1), (8, width))

    pl.semaphore_wait(barrier, (nsmp - 1) + (nsub - 1) + (ntrm - 1))

    def sub_copy(chunk, p, d):
        return pltpu.make_async_remote_copy(
            src_ref=slabs.at[chunk], dst_ref=slabs.at[chunk],
            send_sem=sub_send.at[p, d - 1], recv_sem=recv.at[chunk],
            device_id={"sub": lax.rem(sub + d, nsub)}, device_id_type=MESH,
        )

    def ici_copy(d):
        return pltpu.make_async_remote_copy(
            src_ref=slabs.at[me], dst_ref=slabs.at[me],
            send_sem=ici_send.at[d - 1], recv_sem=recv.at[me],
            device_id={"smp": xor_index(smp, d, nsmp)}, device_id_type=MESH,
        )

    def code_copy(d):
        return pltpu.make_async_remote_copy(
            src_ref=codes_in.at[trm], dst_ref=codes_in.at[trm],
            send_sem=code_send.at[d - 1], recv_sem=code_recv.at[trm],
            device_id={"trm": lax.rem(trm + d, ntrm)}, device_id_type=MESH,
        )

    def wait_slab(chunk):
        pltpu.make_async_remote_copy(
            src_ref=slabs.at[chunk], dst_ref=slabs.at[chunk],
            send_sem=ici_send.at[0], recv_sem=recv.at[chunk],
            device_id={"sub": lax.rem(sub + 1, nsub)}, device_id_type=MESH,
        ).wait_recv()

    for d in range(1, nsmp):
        ici_copy(d).start()
    for d in range(1, nsub):
        sub_copy(me, 0, d).start()
    for d in range(1, ntrm):
        code_copy(d).start()

    def chunk_of(p, s):
        return xor_index(smp, p, nsmp) * nsub + lax.rem(sub + s, nsub)

    def pick(ta, tb, d_ref, begin, end):
        dims = (((1,), (0,)), ((), ()))
        for n in range(0, d_ref.shape[1], 256):
            a = lax.dot_general(sel_a[begin:end, :], ta[:, n : n + 256], dims, preferred_element_type=jnp.float32)
            b = lax.dot_general(sel_b[begin:end, :], tb[:, n : n + 256], dims, preferred_element_type=jnp.float32)
            d_ref[begin:end, n : n + 256] = (a * b).astype(jnp.bfloat16)

    def add(z_ref, d_ref):
        d_ref[selected : selected + 16, :] = z_ref[...]
        for c in range(0, terms, 256):
            e = min(c + 256, terms)
            acc[:, c:e] += lax.dot_general(
                d_ref[terms : selected + 16, :], d_ref[c:e, :], (((1,), (1,)), ((), ())),
                preferred_element_type=jnp.float32,
            )

    def next_own(p):
        following = chunk_of(lax.rem(p + 1, nsmp), 0)

        @pl.when(p + 1 < nsmp)
        def _():
            wait_slab(following)
            for d in range(1, nsub):
                sub_copy(following, p + 1, d).start()

        return slabs[following]

    set0, set1 = (work0, ta0, tb0, z0), (work1, ta1, tb1, z1)

    build_tables(plan, samples_total, slabs[me], *set0)

    def select(row, base, count):
        column = jnp.broadcast_to(row, (128, 128)).T.astype(jnp.int32)[0:count, :]
        for ref, wanted, rows in ((sel_a, column >> 8, plan.rows_a), (sel_b, column & (BASE - 1), plan.rows_b)):
            for j in range(0, ref.shape[1], 128):
                lane = lax.rem(lax.broadcasted_iota(jnp.int32, (count, 128), 1) + j, rows)
                ref[base : base + count, j : j + 128] = (wanted == lane).astype(jnp.bfloat16)

    for i in range(0, terms, 128):
        count = min(128, terms - i)
        row = code[:, i : i + count].astype(jnp.float32)
        if count < 128:
            row = jnp.concatenate([row, jnp.zeros((1, 128 - count), jnp.float32)], axis=1)
        select(row, i, count)

    partner = chunk_of(0, 1)
    pick(ta0, tb0, d0, 0, terms)
    wait_slab(partner)
    build_tables(plan, samples_total, slabs[partner], *set1)
    pick(ta1, tb1, d1, 0, terms)

    for d in range(1, ntrm):
        other = lax.rem(trm + d, ntrm)
        pltpu.make_async_remote_copy(
            src_ref=codes_in.at[other], dst_ref=codes_in.at[other],
            send_sem=code_send.at[d - 1], recv_sem=code_recv.at[other],
            device_id={"trm": other}, device_id_type=MESH,
        ).wait_recv()
    wanted = codes_in[me // per_trm]
    for i in range(0, right, 128):
        select(wanted[0:1, i : i + 128], terms + i, min(128, right - i))
    pick(ta0, tb0, d0, terms, selected)

    add(z0, d0)
    following = next_own(0)
    pick(ta1, tb1, d1, terms, selected)
    add(z1, d1)
    build_tables(plan, samples_total, following, *set0)

    def body(p, carry):
        second = chunk_of(p, 1)
        wait_slab(second)
        pick(ta0, tb0, d0, 0, selected)
        add(z0, d0)
        build_tables(plan, samples_total, slabs[second], *set1)
        following = next_own(p)
        pick(ta1, tb1, d1, 0, selected)
        add(z1, d1)
        build_tables(plan, samples_total, following, *set0)
        return carry

    lax.fori_loop(1, nsmp, body, 0)

    for d in range(1, ntrm):
        code_copy(d).wait_send()
    for d in range(1, nsmp):
        ici_copy(d).wait_send()
    for p in range(nsmp):
        for d in range(1, nsub):
            sub_copy(chunk_of(p, 0), p, d).wait_send()


def write_out(columns, acc_ref, gram_out, rhs_out, flat, sem):
    copy = pltpu.make_async_copy(acc_ref.at[0 : gram_out.shape[0], :], gram_out, sem.at[0])
    copy.start()
    z = up(columns, 16)
    terms = acc_ref.shape[1]
    line = acc_ref[z : z + 1, :] + acc_ref[z + 1 : z + 2, :]
    line = jnp.concatenate([line, jnp.zeros((1, flat.shape[0] - terms), jnp.float32)], axis=1)
    rows = [line[:, i : i + 128] for i in range(0, flat.shape[0], 128)]
    flat[...] = jnp.concatenate(rows, axis=0).reshape(flat.shape)
    tail = pltpu.make_async_copy(flat.at[pl.ds(0, rhs_out.shape[0])], rhs_out, sem.at[1])
    tail.start()
    tail.wait()
    copy.wait()


def solution(mesh):
    nsmp, nsub, ntrm = mesh.shape["smp"], mesh.shape["sub"], mesh.shape["trm"]

    def local(inputs, weights, response, index_table):
        nin, samples = inputs.shape
        terms = index_table.shape[1]
        columns = terms * ntrm // (nsmp * nsub)
        plan = Plan(nin)
        right = up(columns, 16)
        width = up(columns, 128)
        chunks = nsmp * nsub
        acc = pl.pallas_call(
            functools.partial(kernel, plan, (nsmp, nsub, ntrm), columns, samples * chunks),
            out_shape=pltpu.VMEM((right + 16, terms), jnp.float32),
            in_specs=[pl.BlockSpec(memory_space=pltpu.HBM)] * 4,
            out_specs=pl.BlockSpec(memory_space=pltpu.VMEM),
            scratch_shapes=[
                pltpu.VMEM((chunks, 16, plan.groups * samples // 2), jnp.int16),
                pltpu.VMEM((nin, samples), jnp.float32),
                pltpu.VMEM((1, samples), jnp.float32),
                pltpu.VMEM((1, samples), jnp.float32),
                pltpu.VMEM((nin, terms), jnp.int32),
                pltpu.VMEM((ntrm, 8, width), jnp.float32),
                pltpu.VMEM((terms + right, 2 * plan.rows_a), jnp.bfloat16),
                pltpu.VMEM((terms + right, 2 * plan.rows_b), jnp.bfloat16),
            ]
            + [
                pltpu.VMEM((2 * plan.rows_a, samples), jnp.bfloat16),
                pltpu.VMEM((2 * plan.rows_b, samples), jnp.bfloat16),
                pltpu.VMEM((16, samples), jnp.bfloat16),
            ]
            * 2
            + [pltpu.VMEM((plan.rows_b, samples), jnp.float32)] * 2
            + [pltpu.VMEM((terms + right + 16, samples), jnp.bfloat16)] * 2
            + [
                pltpu.SemaphoreType.DMA((4,)),
                pltpu.SemaphoreType.DMA((max(nsmp - 1, 1),)),
                pltpu.SemaphoreType.DMA((nsmp, max(nsub - 1, 1))),
                pltpu.SemaphoreType.DMA((chunks,)),
                pltpu.SemaphoreType.DMA((max(ntrm - 1, 1),)),
                pltpu.SemaphoreType.DMA((ntrm,)),
            ],
            compiler_params=pltpu.CompilerParams(
                collective_id=0, has_side_effects=True, vmem_limit_bytes=40 * 1024 * 1024
            ),
        )(*map(
            lambda v: pltpu.with_memory_space_constraint(v, pltpu.HBM),
            (inputs, weights.reshape(1, samples), response.reshape(1, samples), index_table),
        ))
        gram, rhs = pl.pallas_call(
            functools.partial(write_out, columns),
            out_shape=(
                jax.ShapeDtypeStruct((up(columns, 8), terms), jnp.float32),
                jax.ShapeDtypeStruct((up(terms, 1024) if terms % 128 else terms,), jnp.float32),
            ),
            in_specs=[pl.BlockSpec(memory_space=pltpu.VMEM)],
            out_specs=(pl.BlockSpec(memory_space=pl.ANY),) * 2,
            scratch_shapes=[
                pltpu.VMEM((up(terms, 1024),), jnp.float32),
                pltpu.SemaphoreType.DMA((2,)),
            ],
        )(pltpu.with_memory_space_constraint(acc, pltpu.VMEM))
        return gram[0:columns].T, rhs[0:terms]

    return jax.shard_map(
        local,
        mesh=mesh,
        in_specs=(
            P(None, ("grp", "smp", "sub")),
            P(("grp", "smp", "sub")),
            P(("grp", "smp", "sub")),
            P(None, "trm"),
        ),
        out_specs=(P(("grp", "trm"), ("smp", "sub")), P(("grp", "trm"))),
        check_vma=False,
    )
```
